32 devices in a mesh: section: 4 (over y, core), row: 2 (over x), col: 4 (over z).
Axes of the slice: x: 2, y: 2, z: 4, core: 2. Of those that a mesh axis runs over, the one named last changes fastest.
Arguments:
- weights: bfloat16 [4, 6144, 6144], P('section', ('row', 'col')), may hold values from -0.109375 to 0.109375
- acts: bfloat16 [4, 4, 6144, 128], P('section', None, ('row', 'col')), may hold values from -6 to 6
- grads: bfloat16 [4, 4, 6144, 128], P('section', None, ('row', 'col')), may hold values from -6 to 6
- saved: bfloat16 [4, 4, 6144, 128], P('section', None, ('row', 'col')), may hold values from -6 to 6
- plan: int32 [4, 2, 2], P('section'), may hold values from 0 to 3
Outputs:
- new_acts: bfloat16 [4, 4, 6144, 128], P('section', None, ('row', 'col'))
- new_grads: bfloat16 [4, 4, 6144, 128], P('section', None, ('row', 'col'))
The draws below stay inside these ranges and needn't reach their ends.
Inputs may be any that keep to these rules, and one draw needn't show every extreme that they name: plan[s, t, 0] is the slot read by section s's forward step in turn t and written by what arrives from section s - 1; plan[s, t, 1] likewise for the backward step and section s + 1.
All inputs are finite; a program needn't handle non-finite values.
Results may differ from the reference program's by a relative error of at most 0.017.
Values may be sent and summed in bfloat16 or wider, within the bound.
A program may use at most 64 MiB of HBM per device.

```python
import jax
import jax.numpy as jnp
from jax import lax

D = 6144
MB = 128
SLOTS = 4
TICKS = 2
SECTIONS = 4
GRID = 8


def place_ends(result, own_key, smallest, high):
    index_at = [jax.random.randint(jax.random.fold_in(own_key, axis), (), 0, length) for axis, length in enumerate(result.shape)]
    longest = result.shape.index(max(result.shape))
    next_to = index_at[:longest] + [(index_at[longest] + 1) % result.shape[longest]] + index_at[longest + 1:]
    return result.at[tuple(index_at)].set(smallest).at[tuple(next_to)].set(high)


def with_spikes(drawn, stream_key, source, target, blocks, factor):
    owner, partner = [(jnp.arange(drawn.shape[position]) // (drawn.shape[position] // blocks)).reshape([-1 if axis == position else 1 for axis in range(drawn.ndim)]) for position in (source, target)]
    chosen = jax.random.permutation(stream_key, blocks)[partner]
    strong = (owner == chosen) | (owner == (partner + blocks // 2) % blocks)
    return jnp.where(strong, factor * drawn, drawn)


def level_of(own_key, shape, split, low, high):
    def one(dim, shards_of):
        heights = jax.random.uniform(jax.random.fold_in(jax.random.fold_in(own_key, 6), dim), (shards_of,), jnp.float32, low / len(split), high / len(split))
        return jnp.repeat(jnp.exp(heights), shape[dim] // shards_of).reshape((-1,) + (1,) * (len(shape) - dim - 1))

    loudness = one(*split[0])
    for cut in split[1:]:
        loudness = loudness * one(*cut)
    return loudness


def noise(rng, extent, spread, bound, shards=(), held_as=jnp.bfloat16):
    entries = jax.random.normal(rng, extent, jnp.float32) * spread
    if len(shards) > 0:
        entries = level_of(rng, extent, shards, -0.22, 0.18) * entries
    return jnp.clip(entries, min=-bound, max=bound).astype(held_as)


def gaussian_with(rng, extent, deviation, limit, cuts, heavy, kind=jnp.bfloat16):
    entries = deviation * jax.random.normal(rng, extent, jnp.float32)
    if cuts:
        entries = entries * level_of(rng, extent, cuts, -0.22, 0.18)
    return jnp.clip(with_spikes(entries, jax.random.fold_in(rng, 3), *heavy), -limit, limit).astype(kind)


def setup_inputs(seed: int = 0) -> dict:
    key_list = jax.random.split(jax.random.key(seed), 6)
    return {
        "weights": gaussian_with(key_list[0], (SECTIONS, D, D), D ** -0.5, 0.109375, ((0, 4), (1, 8)), (1, 2, 8, 2.0)),
        "acts": noise(key_list[1], (SECTIONS, SLOTS, D, MB), 1.0, 6.0, ((0, 4), (2, 8))),
        "grads": noise(key_list[2], (SECTIONS, SLOTS, D, MB), 1.0, 6.0, ((0, 4), (2, 8))),
        "saved": noise(key_list[3], (SECTIONS, SLOTS, D, MB), 1.0, 6.0, ((0, 4), (2, 8))),
        "plan": place_ends(jax.random.randint(key_list[4], (SECTIONS, TICKS, 2), 0, SLOTS), jax.random.fold_in(key_list[4], 1), 0, SLOTS - 1).astype(jnp.int32),
    }


def gelu_tanh(values):
    return jax.nn.gelu(values, approximate=True)

def forward_layer(paired):
    weight, inputs = paired
    grouped_weight = weight.reshape(GRID, D // GRID, D).astype(jnp.float32)
    grouped_inputs = inputs.reshape(GRID, D // GRID, MB).astype(jnp.float32)
    partial_value = jnp.einsum('gkn,gkm->gnm', grouped_weight, grouped_inputs).astype(jnp.bfloat16)
    partial_value = lax.optimization_barrier(partial_value)
    summed = lax.optimization_barrier(jnp.sum(partial_value.astype(jnp.float32), axis=0))
    return (inputs.astype(jnp.float32) + gelu_tanh(summed)).astype(jnp.bfloat16)

def backward_layer(tripled):
    weight, upstream, stored = tripled
    upstream_wide = upstream.astype(jnp.float32)
    slope_term = jax.vjp(gelu_tanh, stored.astype(jnp.float32))[1](upstream_wide)[0]
    scaled = slope_term.astype(jnp.bfloat16)
    carried = jnp.dot(weight, scaled, preferred_element_type=jnp.float32)
    return (upstream_wide + carried).astype(jnp.bfloat16)

def reference(weights, acts, grads, saved, plan):
    section_ids = jnp.arange(SECTIONS, dtype=jnp.int32)
    for turn_index in range(TICKS):
        front_slot = plan[:, turn_index, 0].astype(jnp.int32)
        back_slot = plan[:, turn_index, 1].astype(jnp.int32)
        inputs = acts[section_ids, front_slot]
        upstream = grads[section_ids, back_slot]
        stored = saved[section_ids, back_slot]
        outputs = lax.map(forward_layer, (weights, inputs))
        returned = lax.map(backward_layer, (weights, upstream, stored))
        acts = acts.at[section_ids, front_slot].set(jnp.roll(outputs, 1, axis=0))
        grads = grads.at[section_ids, back_slot].set(jnp.roll(returned, -1, axis=0))
    return (acts, grads)
```

```python
import functools

import jax
import jax.numpy as jnp
from jax import lax
from jax.experimental import pallas as pl
from jax.experimental.pallas import tpu as pltpu
from jax.sharding import PartitionSpec as P

TICKS = 2
MESH = pl.DeviceIdType.MESH
ROOT = 0.7978845608028654
CUBE = 0.044715


def from_behind(block, axis, distance):
    devices = range(lax.axis_size(axis))
    route = [((i - distance) % len(devices), i) for i in devices]
    return lax.ppermute(block, axis, route)


def gelu_tanh(values):
    return jax.nn.gelu(values, approximate=True)


def plain_shards(weights, acts, grads, saved, plan):
    weight = weights[0]
    held_inputs = acts[0]
    held_grads = grads[0]
    held_saved = saved[0]
    slot_table = plan[0]
    for turn_index in range(TICKS):
        front_slot = slot_table[turn_index, 0]
        back_slot = slot_table[turn_index, 1]
        inputs = lax.dynamic_index_in_dim(held_inputs, front_slot, 0, keepdims=False)
        upstream = lax.dynamic_index_in_dim(held_grads, back_slot, 0, keepdims=False)
        stored_preact = lax.dynamic_index_in_dim(held_saved, back_slot, 0, keepdims=False)
        row_block = lax.psum_scatter(
            lax.dot_general(
                weight, inputs, (((0,), (0,)), ((), ())), preferred_element_type=jnp.float32
            ).astype(jnp.bfloat16),
            "row",
            scatter_dimension=0,
            tiled=True,
        )
        summed = lax.psum_scatter(row_block, "col", scatter_dimension=0, tiled=True).astype(
            jnp.float32
        )
        outputs = (inputs.astype(jnp.float32) + gelu_tanh(summed)).astype(jnp.bfloat16)
        upstream_wide = upstream.astype(jnp.float32)
        slope_term = jax.vjp(gelu_tanh, stored_preact.astype(jnp.float32))[1](upstream_wide)[0]
        scaled = slope_term.astype(jnp.bfloat16)
        carried = jnp.dot(
            weight,
            lax.all_gather(scaled, ("row", "col"), axis=0, tiled=True),
            preferred_element_type=jnp.float32,
        )
        returned = (upstream_wide + carried).astype(jnp.bfloat16)
        arrived = from_behind(outputs, "section", 1)
        sent_back = from_behind(returned, "section", -1)
        held_inputs = lax.dynamic_update_index_in_dim(held_inputs, arrived, front_slot, 0)
        held_grads = lax.dynamic_update_index_in_dim(held_grads, sent_back, back_slot, 0)
    return (held_inputs[None], held_grads[None])


def gelu_slope(v):
    t = jnp.tanh(ROOT * (v + CUBE * (v * v * v)))
    return 0.5 * (1.0 + t) + 0.5 * v * (1.0 - t * t) * (ROOT * (1.0 + 3.0 * CUBE * (v * v)))


def gelu_value(v):
    return 0.5 * v * (1.0 + jnp.tanh(ROOT * (v + CUBE * (v * v * v))))


def relay_kernel(S, X, Z, cut, plan, w_any, acts, grads, saved, new_y, new_r,
                 w, wsem, ups, slopes, xt, own, racc, out_x, in_x, out_z, in_z, y_out, r_out,
                 y_in, r_in, ga_s, gb_s, gline_s, g_r, rx_s, rx_r, rz_s, rz_r, sh_s, sh_r):
    s, x, z = lax.axis_index("section"), lax.axis_index("row"), lax.axis_index("col")
    n = X * Z
    me = x * Z + z
    blk, mb = acts.shape[2], acts.shape[3]
    f32, bf16 = jnp.float32, jnp.bfloat16
    up_ok, down_ok = z < Z - 1, z > 0
    pending = []

    def w_copy(j):
        return pltpu.make_async_copy(
            w_any.at[0, :, pl.ds(j * blk, blk)], w.at[j], wsem.at[j])

    for j in range(n):
        w_copy(j).start()

    barrier = pltpu.get_barrier_semaphore()
    for k in range(1, X):
        pl.semaphore_signal(barrier, 1, device_id={"row": lax.rem(x + k, X)}, device_id_type=MESH)
    for k in (1, S - 1):
        pl.semaphore_signal(barrier, 1, device_id={"section": lax.rem(s + k, S)}, device_id_type=MESH)

    @pl.when(up_ok)
    def _():
        pl.semaphore_signal(barrier, 1, device_id={"col": z + 1}, device_id_type=MESH)

    @pl.when(down_ok)
    def _():
        pl.semaphore_signal(barrier, 1, device_id={"col": z - 1}, device_id_type=MESH)

    pl.semaphore_wait(barrier, X + 1 + (1 - (z + 1) // Z) + (z + Z - 1) // Z)

    def remote(src, dst, ssem, rsem, where):
        return pltpu.make_async_remote_copy(
            src_ref=src, dst_ref=dst, send_sem=ssem, recv_sem=rsem,
            device_id=where, device_id_type=MESH)

    def send(make, cond=None):
        pending.append((make, cond))
        if cond is None:
            make().start()
        else:
            pl.when(cond)(lambda: make().start())

    A, B = (0, cut), (cut, blk)

    def piece(t, p, j):
        lo, hi = (A, B)[p]
        return slopes.at[t, j, lo:hi, :]

    def line(t, p, j, step):
        ref = piece(t, p, j)
        return remote(ref, ref, gline_s.at[t, p, (step + 1) // 2, j], g_r.at[t, p, j],
                      {"col": z + step})

    def across(t, p, j, k):
        ref = piece(t, p, j)
        sem = ga_s.at[t, k - 1, lax.rem(j, Z)] if p == 0 else gb_s.at[t, k - 1]
        return remote(ref, ref, sem, g_r.at[t, p, j], {"row": lax.rem(x + k, X)})

    def got(t, p, j):
        ref = piece(t, p, j)
        pltpu.make_async_copy(ref, ref, g_r.at[t, p, j]).wait()

    def order(i):
        b = (i + z + 1) // Z
        return (1 - b) * (Z - 1 - i) + b * (i - (Z - 1 - z))

    def slot(t, which):
        return plan[0, t, which]

    def pick(t, which, ref, arrived):
        base = ref[0, slot(t, which)]
        for u in range(t):
            hit = jnp.full(base.shape, slot(u, which) - slot(t, which), jnp.int32) == 0
            base = jnp.where(hit, arrived[u].astype(f32), base.astype(f32)).astype(bf16)
        return base

    def gather_start(t):
        upstream = pick(t, 1, grads, r_in)
        ups[t] = upstream
        slopes[t, me] = (upstream.astype(f32) * gelu_slope(saved[0, slot(t, 1)].astype(f32))).astype(bf16)
        for p in (0, 1):
            send(functools.partial(line, t, p, me, 1), up_ok)
            send(functools.partial(line, t, p, me, -1), down_ok)
            if p == 0:
                for k in range(1, X):
                    send(functools.partial(across, t, 1, me, k))
        for k in range(1, X):
            send(functools.partial(across, t, 0, me, k))

    def gather_partner(t):
        for k in range(1, X):
            j = lax.rem(x + k, X) * Z + z
            got(t, 1, j)
            send(functools.partial(line, t, 1, j, 1), up_ok)
            send(functools.partial(line, t, 1, j, -1), down_ok)

    def gather_stage(t, d):
        for step, there in ((1, z >= d), (-1, z + d < Z)):
            zs = z - step * d
            on = (z >= d) & up_ok if step == 1 else (z + d < Z) & down_ok

            def take(p, j):
                pl.when(there)(lambda: got(t, p, j))
                send(functools.partial(line, t, p, j, step), on)

            mine = x * Z + zs
            take(0, mine)
            for k in range(1, X):
                send(functools.partial(across, t, 0, mine, k), there)
            for k in range(X):
                take(1, lax.rem(x + k, X) * Z + zs)

    def gather_finish(t):
        for k in range(1, X):
            for zs in range(Z):
                got(t, 0, lax.rem(x + k, X) * Z + zs)
        racc[...] = ups[t].astype(f32)

        @pl.loop(0, n)
        def _(j):
            racc[...] += jnp.dot(w[j], slopes[t, j], preferred_element_type=f32)

        r_out[t] = racc[...].astype(bf16)
        send(lambda: remote(r_out.at[t], r_in.at[t], sh_s.at[t, 1], sh_r.at[t, 1],
                            {"section": lax.rem(s + S - 1, S)}))

    def row_copy(t, k, i):
        return remote(out_x.at[t, k - 1, i], in_x.at[t, k - 1, i], rx_s.at[t, k - 1, i],
                      rx_r.at[t, k - 1, i], {"row": lax.rem(x + k, X)})

    def forward_products(t):
        inputs = pick(t, 0, acts, y_in)
        xt[...] = inputs.astype(f32).T.astype(bf16)

        def product(j):
            return jnp.dot(xt[...], w[j], preferred_element_type=f32)

        for k in range(1, X):
            @pl.loop(0, Z)
            def _(i):
                out_x[t, k - 1, i] = product(lax.rem(x + k, X) * Z + order(i)).astype(bf16)

                @pl.when(i < 2)
                def _():
                    row_copy(t, k, i).start()
            for i in range(2):
                pending.append((functools.partial(row_copy, t, k, i), None))

        @pl.loop(0, Z)
        def _(i):
            own[i] = product(x * Z + order(i))

    def row_send(t, i):
        for k in range(1, X):
            send(functools.partial(row_copy, t, k, i))

    def line_sum(t, step, i):
        d = (step + 1) // 2
        return remote(out_z.at[t, i], in_z.at[t, d, i if step == 1 else i + 1],
                      rz_s.at[t, i], rz_r.at[t, d, i if step == 1 else i + 1], {"col": z + step})

    def sum_arrival(t, d, i):
        ref = in_z.at[t, d, i]
        pltpu.make_async_copy(ref, ref, rz_r.at[t, d, i]).wait()
        own[i] += in_z[t, d, i].astype(f32)

    def sum_stage(t, i):
        for k in range(1, X):
            ref = in_x.at[t, k - 1, i]
            pltpu.make_async_copy(ref, ref, rx_r.at[t, k - 1, i]).wait()
        total = own[i]
        for k in range(1, X):
            total = total + in_x[t, k - 1, i].astype(f32)
        own[i] = total
        if i < Z - 1:
            up = z + i + 1 < Z
            down = z + i + 1 >= Z

            @pl.when(up & down_ok)
            def _():
                sum_arrival(t, 1, i)

            @pl.when(down & up_ok)
            def _():
                sum_arrival(t, 0, i)

            out_z[t, i] = own[i].astype(bf16)
            send(functools.partial(line_sum, t, 1, i), up)
            send(functools.partial(line_sum, t, -1, i), down)
        else:
            for zz in range(Z):
                @pl.when(z == zz)
                def _(zz=zz):
                    for d, idx in ((1, Z - 1 - zz), (0, Z - 1)):
                        if (d == 1 and zz > 0) or (d == 0 and zz < Z - 1):
                            ref = in_z.at[t, d, idx]
                            pltpu.make_async_copy(ref, ref, rz_r.at[t, d, idx]).wait()
                            own[i] += in_z[t, d, idx].astype(f32)
            inputs = pick(t, 0, acts, y_in)
            gate = gelu_value(own[i]).T
            y_out[t] = (inputs.astype(f32) + gate).astype(bf16)
            send(lambda: remote(y_out.at[t], y_in.at[t], sh_s.at[t, 0], sh_r.at[t, 0],
                                {"section": lax.rem(s + 1, S)}))

    def shifted(t, which):
        ref = (y_in, r_in)[which].at[t]
        pltpu.make_async_copy(ref, ref, sh_r.at[t, which]).wait()

    gather_start(0)
    for j in range(n):
        w_copy(j).wait()
    for t in range(TICKS):
        forward_products(t)
        gather_partner(t)
        for d in range(1, Z):
            gather_stage(t, d)
            if d + 1 < Z:
                row_send(t, d + 1)
            if d < Z - 1:
                sum_stage(t, d - 1)
        gather_finish(t)
        sum_stage(t, Z - 2)
        if t + 1 < TICKS:
            shifted(t, 1)
            gather_start(t + 1)
        sum_stage(t, Z - 1)
        shifted(t, 0)
    shifted(TICKS - 1, 1)
    for t in range(TICKS):
        new_y[t] = y_in[t]
        new_r[t] = r_in[t]
    for make, cond in pending:
        if cond is None:
            make().wait_send()
        else:
            pl.when(cond)(lambda make=make: make().wait_send())


def relay_shards(S, X, Z, weights, acts, grads, saved, plan):
    blk, mb = acts.shape[2], acts.shape[3]
    n = X * Z
    cut = blk // 48 * 16
    bf16, f32 = jnp.bfloat16, jnp.float32
    dma = pltpu.SemaphoreType.DMA
    vm = pl.BlockSpec(memory_space=pltpu.VMEM)
    T = TICKS
    new_y, new_r = pl.pallas_call(
        functools.partial(relay_kernel, S, X, Z, cut),
        out_shape=[jax.ShapeDtypeStruct((T, blk, mb), bf16)] * 2,
        in_specs=[pl.BlockSpec(memory_space=pltpu.SMEM), pl.BlockSpec(memory_space=pl.ANY), vm, vm, vm],
        out_specs=[vm, vm],
        scratch_shapes=[
            pltpu.VMEM((n, blk, blk), bf16),
            dma((n,)),
            pltpu.VMEM((T, blk, mb), bf16),
            pltpu.VMEM((T, n, blk, mb), bf16),
            pltpu.VMEM((mb, blk), bf16),
            pltpu.VMEM((Z, mb, blk), f32),
            pltpu.VMEM((blk, mb), f32),
            pltpu.VMEM((T, X - 1, Z, mb, blk), bf16),
            pltpu.VMEM((T, X - 1, Z, mb, blk), bf16),
            pltpu.VMEM((T, Z, mb, blk), bf16),
            pltpu.VMEM((T, 2, Z, mb, blk), bf16),
            pltpu.VMEM((T, blk, mb), bf16),
            pltpu.VMEM((T, blk, mb), bf16),
            pltpu.VMEM((T, blk, mb), bf16),
            pltpu.VMEM((T, blk, mb), bf16),
            dma((T, X - 1, Z)),
            dma((T, X - 1)),
            dma((T, 2, 2, n)),
            dma((T, 2, n)),
            dma((T, X - 1, Z)),
            dma((T, X - 1, Z)),
            dma((T, Z)),
            dma((T, 2, Z)),
            dma((T, 2)),
            dma((T, 2)),
        ],
        compiler_params=pltpu.CompilerParams(
            collective_id=0, has_side_effects=True, vmem_limit_bytes=60000 * 1024
        ),
    )(plan, weights, acts, grads, saved)
    slots = lax.broadcasted_iota(jnp.int32, (1, acts.shape[1], 1, 1), 1)
    for t in range(T):
        acts = jnp.where(slots == plan[0, t, 0], new_y[t], acts)
        grads = jnp.where(slots == plan[0, t, 1], new_r[t], grads)
    return acts, grads


def solution(mesh):
    S, X, Z = (mesh.shape[a] for a in ("section", "row", "col"))

    def shards(weights, acts, grads, saved, plan):
        if acts.shape[2] % 128 == 0 and min(S, X, Z) > 1 and S > 2:
            return relay_shards(S, X, Z, weights, acts, grads, saved, plan)
        return plain_shards(weights, acts, grads, saved, plan)

    return jax.shard_map(
        shards,
        mesh=mesh,
        in_specs=(
            P("section", ("row", "col"), None),
            P("section", None, ("row", "col"), None),
            P("section", None, ("row", "col"), None),
            P("section", None, ("row", "col"), None),
            P("section", None, None),
        ),
        out_specs=(
            P("section", None, ("row", "col"), None),
            P("section", None, ("row", "col"), None),
        ),
        check_vma=False,
    )
```

```python
import functools

import jax
import jax.numpy as jnp
from jax import lax
from jax.experimental import pallas as pl
from jax.experimental.pallas import tpu as pltpu
from jax.sharding import PartitionSpec as P

TICKS = 2
MESH = pl.DeviceIdType.MESH
ROOT = 0.7978845608028654
CUBE = 0.044715


def from_behind(block, axis, distance):
    devices = range(lax.axis_size(axis))
    route = [((i - distance) % len(devices), i) for i in devices]
    return lax.ppermute(block, axis, route)


def gelu_tanh(values):
    return jax.nn.gelu(values, approximate=True)


def plain_shards(weights, acts, grads, saved, plan):
    weight = weights[0]
    held_inputs = acts[0]
    held_grads = grads[0]
    held_saved = saved[0]
    slot_table = plan[0]
    for turn_index in range(TICKS):
        front_slot = slot_table[turn_index, 0]
        back_slot = slot_table[turn_index, 1]
        inputs = lax.dynamic_index_in_dim(held_inputs, front_slot, 0, keepdims=False)
        upstream = lax.dynamic_index_in_dim(held_grads, back_slot, 0, keepdims=False)
        stored_preact = lax.dynamic_index_in_dim(held_saved, back_slot, 0, keepdims=False)
        row_block = lax.psum_scatter(
            lax.dot_general(
                weight, inputs, (((0,), (0,)), ((), ())), preferred_element_type=jnp.float32
            ).astype(jnp.bfloat16),
            "row",
            scatter_dimension=0,
            tiled=True,
        )
        summed = lax.psum_scatter(row_block, "col", scatter_dimension=0, tiled=True).astype(
            jnp.float32
        )
        outputs = (inputs.astype(jnp.float32) + gelu_tanh(summed)).astype(jnp.bfloat16)
        upstream_wide = upstream.astype(jnp.float32)
        slope_term = jax.vjp(gelu_tanh, stored_preact.astype(jnp.float32))[1](upstream_wide)[0]
        scaled = slope_term.astype(jnp.bfloat16)
        carried = jnp.dot(
            weight,
            lax.all_gather(scaled, ("row", "col"), axis=0, tiled=True),
            preferred_element_type=jnp.float32,
        )
        returned = (upstream_wide + carried).astype(jnp.bfloat16)
        arrived = from_behind(outputs, "section", 1)
        sent_back = from_behind(returned, "section", -1)
        held_inputs = lax.dynamic_update_index_in_dim(held_inputs, arrived, front_slot, 0)
        held_grads = lax.dynamic_update_index_in_dim(held_grads, sent_back, back_slot, 0)
    return (held_inputs[None], held_grads[None])


def gelu_slope(v):
    t = jnp.tanh(ROOT * (v + CUBE * (v * v * v)))
    return 0.5 * (1.0 + t) + 0.5 * v * (1.0 - t * t) * (ROOT * (1.0 + 3.0 * CUBE * (v * v)))


def gelu_value(v):
    return 0.5 * v * (1.0 + jnp.tanh(ROOT * (v + CUBE * (v * v * v))))


def relay_kernel(S, X, Z, cut, plan, w_any, acts, grads, saved, *rest):
    new_y, new_r = rest[:TICKS], rest[TICKS : 2 * TICKS]
    (w, wsem, ups, slopes, xt, own, racc, out_x, in_x, out_z, in_z, y_out, r_out,
     y_in, r_in, ga_s, gb_s, gline_s, g_r, rx_s, rx_r, rz_s, rz_r, sh_s, sh_r) = rest[2 * TICKS :]
    s, x, z = lax.axis_index("section"), lax.axis_index("row"), lax.axis_index("col")
    n = X * Z
    me = x * Z + z
    blk, mb = acts.shape[2], acts.shape[3]
    f32, bf16 = jnp.float32, jnp.bfloat16
    up_ok, down_ok = z < Z - 1, z > 0
    pending = []

    def w_copy(j):
        return pltpu.make_async_copy(
            w_any.at[0, :, pl.ds(j * blk, blk)], w.at[j], wsem.at[j])

    for j in range(n):
        w_copy(j).start()

    barrier = pltpu.get_barrier_semaphore()
    for k in range(1, X):
        pl.semaphore_signal(barrier, 1, device_id={"row": lax.rem(x + k, X)}, device_id_type=MESH)
    for k in (1, S - 1):
        pl.semaphore_signal(barrier, 1, device_id={"section": lax.rem(s + k, S)}, device_id_type=MESH)

    @pl.when(up_ok)
    def _():
        pl.semaphore_signal(barrier, 1, device_id={"col": z + 1}, device_id_type=MESH)

    @pl.when(down_ok)
    def _():
        pl.semaphore_signal(barrier, 1, device_id={"col": z - 1}, device_id_type=MESH)

    pl.semaphore_wait(barrier, X + 1 + (1 - (z + 1) // Z) + (z + Z - 1) // Z)

    def remote(src, dst, ssem, rsem, where):
        return pltpu.make_async_remote_copy(
            src_ref=src, dst_ref=dst, send_sem=ssem, recv_sem=rsem,
            device_id=where, device_id_type=MESH)

    def send(make, cond=None):
        pending.append((make, cond))
        if cond is None:
            make().start()
        else:
            pl.when(cond)(lambda: make().start())

    A, B = (0, cut), (cut, blk)

    def piece(t, p, j):
        lo, hi = (A, B)[p]
        return slopes.at[t, j, lo:hi, :]

    def line(t, p, j, step):
        ref = piece(t, p, j)
        return remote(ref, ref, gline_s.at[t, p, (step + 1) // 2, j], g_r.at[t, p, j],
                      {"col": z + step})

    def across(t, p, j, k):
        ref = piece(t, p, j)
        sem = ga_s.at[t, k - 1, lax.rem(j, Z)] if p == 0 else gb_s.at[t, k - 1]
        return remote(ref, ref, sem, g_r.at[t, p, j], {"row": lax.rem(x + k, X)})

    def got(t, p, j):
        ref = piece(t, p, j)
        pltpu.make_async_copy(ref, ref, g_r.at[t, p, j]).wait()

    def order(i):
        half = (2 * z) // Z
        low = (1 - half) * z + half * (Z - 1 - z)
        b = (i + low + 1) // Z
        block = (1 - b) * (Z - 1 - i) + b * (i - (Z - 1 - low))
        return (1 - half) * block + half * (Z - 1 - block)

    def slot(t, which):
        return plan[0, t, which]

    def pick(t, which, ref, arrived):
        base = ref[0, slot(t, which)]
        for u in range(t):
            hit = jnp.full(base.shape, slot(u, which) - slot(t, which), jnp.int32) == 0
            base = jnp.where(hit, arrived[u].astype(f32), base.astype(f32)).astype(bf16)
        return base

    def gather_start(t):
        upstream = pick(t, 1, grads, r_in)
        ups[t] = upstream
        slopes[t, me] = (upstream.astype(f32) * gelu_slope(saved[0, slot(t, 1)].astype(f32))).astype(bf16)
        for p in (0, 1):
            send(functools.partial(line, t, p, me, 1), up_ok)
            send(functools.partial(line, t, p, me, -1), down_ok)
            if p == 0:
                for k in range(1, X):
                    send(functools.partial(across, t, 1, me, k))
        for k in range(1, X):
            send(functools.partial(across, t, 0, me, k))

    def gather_partner(t):
        for k in range(1, X):
            j = lax.rem(x + k, X) * Z + z
            got(t, 1, j)
            send(functools.partial(line, t, 1, j, 1), up_ok)
            send(functools.partial(line, t, 1, j, -1), down_ok)

    def gather_stage(t, d):
        for step, there in ((1, z >= d), (-1, z + d < Z)):
            zs = z - step * d
            on = (z >= d) & up_ok if step == 1 else (z + d < Z) & down_ok

            def take(p, j):
                pl.when(there)(lambda: got(t, p, j))
                send(functools.partial(line, t, p, j, step), on)

            mine = x * Z + zs
            take(0, mine)
            for k in range(1, X):
                send(functools.partial(across, t, 0, mine, k), there)
            for k in range(X):
                take(1, lax.rem(x + k, X) * Z + zs)

    def accumulate(t, d):
        for step in (1, -1) if d else (1,):
            zs = z - step * d

            def add():
                for k in range(1, X):
                    got(t, 0, lax.rem(x + k, X) * Z + zs)

                @pl.loop(0, X)
                def _(k):
                    j = k * Z + zs
                    racc[...] += jnp.dot(w[j], slopes[t, j], preferred_element_type=f32)

            if d:
                pl.when(z >= d if step == 1 else z + d < Z)(add)
            else:
                racc[...] = ups[t].astype(f32)
                add()

    def gather_finish(t):
        r_out[t] = racc[...].astype(bf16)
        send(lambda: remote(r_out.at[t], r_in.at[t], sh_s.at[t, 1], sh_r.at[t, 1],
                            {"section": lax.rem(s + S - 1, S)}))

    def row_copy(t, k, i):
        b = order(i)
        return remote(out_x.at[t, k - 1, b], in_x.at[t, k - 1, b], rx_s.at[t, k - 1, b],
                      rx_r.at[t, k - 1, b], {"row": lax.rem(x + k, X)})

    def product(j):
        return jnp.dot(xt[...], w[j], preferred_element_type=f32)

    def row_products(t):
        inputs = pick(t, 0, acts, y_in)
        xt[...] = inputs.astype(f32).T.astype(bf16)
        for k in range(1, X):
            @pl.loop(0, Z)
            def _(i):
                b = order(i)
                out_x[t, k - 1, b] = product(lax.rem(x + k, X) * Z + b).astype(bf16)

                @pl.when(i < 2)
                def _():
                    row_copy(t, k, i).start()
            for i in range(2):
                pending.append((functools.partial(row_copy, t, k, i), None))

    def own_products(t):
        @pl.loop(0, Z)
        def _(b):
            own[b] = product(x * Z + b)

    def row_send(t, i):
        for k in range(1, X):
            send(functools.partial(row_copy, t, k, i))

    def arrived(ref, sem):
        pltpu.make_async_copy(ref, ref, sem).wait()

    def row_sum(t, b):
        total = own[b]
        for k in range(1, X):
            arrived(in_x.at[t, k - 1, b], rx_r.at[t, k - 1, b])
            total = total + in_x[t, k - 1, b].astype(f32)
        own[b] = total

    def line_add(t, d, level, b):
        arrived(in_z.at[t, d, level], rz_r.at[t, d, level])
        own[b] += in_z[t, d, level].astype(f32)

    def line_copy(t, step, level, b):
        d = (step + 1) // 2
        return remote(out_z.at[t, b], in_z.at[t, d, level + 1], rz_s.at[t, b],
                      rz_r.at[t, d, level + 1], {"col": z + step})

    def sum_level(t, level):
        for step in (1, -1):
            d = (step + 1) // 2
            on = level >= z if step == 1 else level >= Z - 1 - z
            b = Z - 1 - level + z if step == 1 else level - (Z - 1 - z)
            inner = down_ok if step == 1 else up_ok

            @pl.when(on)
            def _():
                row_sum(t, b)
                pl.when(inner)(lambda: line_add(t, d, level, b))
                out_z[t, b] = own[b].astype(bf16)

            send(functools.partial(line_copy, t, step, level, b), on)

    def sum_own(t):
        row_sum(t, z)
        pl.when(down_ok)(lambda: line_add(t, 1, Z - 1, z))
        pl.when(up_ok)(lambda: line_add(t, 0, Z - 1, z))
        inputs = pick(t, 0, acts, y_in)
        y_out[t] = (inputs.astype(f32) + gelu_value(own[z]).T).astype(bf16)
        send(lambda: remote(y_out.at[t], y_in.at[t], sh_s.at[t, 0], sh_r.at[t, 0],
                            {"section": lax.rem(s + 1, S)}))

    def shifted(t, which):
        ref = (y_in, r_in)[which].at[t]
        pltpu.make_async_copy(ref, ref, sh_r.at[t, which]).wait()

    gather_start(0)
    for j in range(n):
        w_copy(j).wait()
    for t in range(TICKS):
        row_products(t)
        gather_partner(t)
        own_products(t)
        for d in range(1, Z):
            gather_stage(t, d)
            if d + 1 < Z:
                row_send(t, d + 1)
            if d < Z - 1:
                sum_level(t, d - 1)
            accumulate(t, d - 1)
        accumulate(t, Z - 1)
        gather_finish(t)
        sum_level(t, Z - 2)
        sum_own(t)
        if t + 1 < TICKS:
            shifted(t, 1)
            gather_start(t + 1)
        shifted(t, 0)
    shifted(TICKS - 1, 1)
    for t in range(TICKS):
        new_y[t][...] = y_in[t]
        new_r[t][...] = r_in[t]
    for make, cond in pending:
        if cond is None:
            make().wait_send()
        else:
            pl.when(cond)(lambda make=make: make().wait_send())


def relay_shards(S, X, Z, weights, acts, grads, saved, plan):
    blk, mb = acts.shape[2], acts.shape[3]
    n = X * Z
    cut = blk // 48 * 16
    bf16, f32 = jnp.bfloat16, jnp.float32
    dma = pltpu.SemaphoreType.DMA
    vm = pl.BlockSpec(memory_space=pltpu.VMEM)
    T = TICKS
    arrivals = pl.pallas_call(
        functools.partial(relay_kernel, S, X, Z, cut),
        out_shape=[jax.ShapeDtypeStruct((blk, mb), bf16)] * (2 * T),
        in_specs=[pl.BlockSpec(memory_space=pltpu.SMEM), pl.BlockSpec(memory_space=pl.ANY), vm, vm, vm],
        out_specs=[vm] * (2 * T),
        scratch_shapes=[
            pltpu.VMEM((n, blk, blk), bf16),
            dma((n,)),
            pltpu.VMEM((T, blk, mb), bf16),
            pltpu.VMEM((T, n, blk, mb), bf16),
            pltpu.VMEM((mb, blk), bf16),
            pltpu.VMEM((Z, mb, blk), f32),
            pltpu.VMEM((blk, mb), f32),
            pltpu.VMEM((T, X - 1, Z, mb, blk), bf16),
            pltpu.VMEM((T, X - 1, Z, mb, blk), bf16),
            pltpu.VMEM((T, Z, mb, blk), bf16),
            pltpu.VMEM((T, 2, Z, mb, blk), bf16),
            pltpu.VMEM((T, blk, mb), bf16),
            pltpu.VMEM((T, blk, mb), bf16),
            pltpu.VMEM((T, blk, mb), bf16),
            pltpu.VMEM((T, blk, mb), bf16),
            dma((T, X - 1, Z)),
            dma((T, X - 1)),
            dma((T, 2, 2, n)),
            dma((T, 2, n)),
            dma((T, X - 1, Z)),
            dma((T, X - 1, Z)),
            dma((T, Z)),
            dma((T, 2, Z)),
            dma((T, 2)),
            dma((T, 2)),
        ],
        compiler_params=pltpu.CompilerParams(
            collective_id=0, has_side_effects=True, vmem_limit_bytes=60000 * 1024
        ),
    )(plan, weights, acts, grads, saved)
    arrivals = lax.optimization_barrier(arrivals)
    for t in range(T):
        acts = lax.dynamic_update_slice(acts, arrivals[t][None, None], (0, plan[0, t, 0], 0, 0))
        grads = lax.dynamic_update_slice(grads, arrivals[T + t][None, None], (0, plan[0, t, 1], 0, 0))
    return acts, grads


def solution(mesh):
    S, X, Z = (mesh.shape[a] for a in ("section", "row", "col"))

    def shards(weights, acts, grads, saved, plan):
        if acts.shape[2] % 128 == 0 and min(S, X, Z) > 1 and S > 2:
            return relay_shards(S, X, Z, weights, acts, grads, saved, plan)
        return plain_shards(weights, acts, grads, saved, plan)

    return jax.shard_map(
        shards,
        mesh=mesh,
        in_specs=(
            P("section", ("row", "col"), None),
            P("section", None, ("row", "col"), None),
            P("section", None, ("row", "col"), None),
            P("section", None, ("row", "col"), None),
            P("section", None, None),
        ),
        out_specs=(
            P("section", None, ("row", "col"), None),
            P("section", None, ("row", "col"), None),
        ),
        check_vma=False,
    )
```
